32 devices in a mesh: group: 2 (over x), grid: 8 (over z, y), var: 2 (over core).
Axes of the slice: x: 2, y: 2, z: 4, core: 2. Of those that a mesh axis runs over, the one named last changes fastest.
Arguments:
- tokens: bfloat16 [96, 96, 3, 512], P('group', 'grid'), parts along dimension 0, may hold values from -6 to 6
- key_mask: int32 [96, 96], P('group', 'grid'), parts along dimension 0, may hold values 0 or 1
- w_qkv: bfloat16 [3, 512, 512], P(None, None, 'var'), may hold values from -16 to 16
- w_proj: bfloat16 [512, 512], P('var'), may hold values from -0.25 to 0.25
- w_up: bfloat16 [512, 2048], P(None, 'var'), may hold values from -0.25 to 0.25
- w_down: bfloat16 [2048, 512], P('var'), may hold values from -0.125 to 0.125
- level_query: bfloat16 [13, 512], replicated, may hold values from -1200 to 1200
- w_dec_q: bfloat16 [512, 512], P(None, 'var'), may hold values from -0.25 to 0.25
- w_dec_kv: bfloat16 [2, 512, 512], P(None, None, 'var'), may hold values from -0.25 to 0.25
- w_dec_o: bfloat16 [512, 512], P('var'), may hold values from -0.25 to 0.25
- decode_matrix: float32 [512, 64], replicated, may hold values from -0.25 to 0.25
Outputs:
- estimated_maps: float32 [4, 26, 192, 384], P('var', 'group', 'grid'), parts along dimension 1
The draws below stay inside these ranges and needn't reach their ends.
There are 2 independent parts, one for each index of `group`. The reference program is written for one: setup_inputs(seed, part) draws one part's arguments, and reference() takes and returns one part's arrays. A program takes and returns all parts, laid end to end along the dimension named above; an argument that names none is the same for every part. Nothing has to cross between parts.
All inputs are finite; a program needn't handle non-finite values. No bound on the sum of `key_mask` on one device may be relied on, other than what follows from the above.
Results may differ from the reference program's by a relative error of at most 0.025.
Values may be sent and summed in bfloat16 or wider, within the bound.
A program may use at most 128 MiB of HBM per device.

```python
import jax
import jax.numpy as jnp
from jax import lax

EMBED_WIDTH = 512
HD = 64
FF = 2048
TARGET_QUANTITY = 4
ISOBAR_NUMBER = 13
LEV = 3
SQUARE_SPAN = 4
WIN_LAT = 6
WINDOW_EASTWARD = 12
LAT = 48
LON = 96


def draw_w_qkv(key, part):
    key = jax.random.fold_in(key, 11)
    base_key = jax.random.fold_in(key, 0)
    result = jnp.clip(jax.random.normal(base_key, (3, EMBED_WIDTH, EMBED_WIDTH), jnp.float32), -6.0, 6.0) * EMBED_WIDTH ** (-0.5)
    return result.astype(jnp.bfloat16)


def draw_level_query(key, part):
    key = jax.random.fold_in(key, 23)
    base_key = jax.random.fold_in(key, 0)
    result = jnp.clip(jax.random.normal(base_key, (ISOBAR_NUMBER, EMBED_WIDTH), jnp.float32), -6.0, 6.0)
    return result.astype(jnp.bfloat16)


def touch_ends(array, rng, smallest, top_value):
    shape = array.shape
    spot = [jax.random.randint(jax.random.fold_in(rng, axis), (), 0, shape[axis]) for axis in range(len(shape))]
    array = array.at[tuple(spot)].set(smallest)
    longest = shape.index(max(shape))
    spot[longest] = (spot[longest] + 1) % shape[longest]
    return array.at[tuple(spot)].set(top_value)


def shard_levels(key, shape, pieces, low, high):
    level, own = 1.0, jax.random.fold_in(key, 6)
    for dim, blocks in pieces:
        heights = jnp.exp(jax.random.uniform(jax.random.fold_in(own, dim), (blocks,), jnp.float32, low / len(pieces), high / len(pieces)))
        level = level * jnp.repeat(heights, shape[dim] // blocks).reshape([-1 if axis == dim else 1 for axis in range(len(shape))])
    return level


def normal_values(key, dims, scale, bound, cuts=(), dtype=jnp.bfloat16):
    level = shard_levels(key, dims, cuts, -0.22, 0.18) if cuts else 1.0
    entries = jax.random.normal(key, dims, jnp.float32) * scale * level
    return jnp.minimum(jnp.maximum(entries, -bound), bound).astype(dtype)


def setup_inputs(seed: int = 0, part: int = 0) -> dict:
    streams_of = jax.random.split(jax.random.key(seed), 12)
    part_splits = jax.random.split(jax.random.fold_in(streams_of[11], part), 12)
    return {
        "tokens": normal_values(part_splits[0], (LAT, LON, LEV, EMBED_WIDTH), 1.0, 6.0, ((1, 8),)),
        "key_mask": touch_ends((jax.random.randint(part_splits[1], (LAT, LON), 0, 4) < 3).astype(jnp.int32), jax.random.fold_in(part_splits[1], 1), 0, 1),
        "w_qkv": draw_w_qkv(jax.random.fold_in(streams_of[11], 71), part),
        "w_proj": normal_values(streams_of[3], (EMBED_WIDTH, EMBED_WIDTH), EMBED_WIDTH ** -0.5, 0.25, ((0, 2),)),
        "w_up": normal_values(streams_of[4], (EMBED_WIDTH, FF), EMBED_WIDTH ** -0.5, 0.25, ((1, 2),)),
        "w_down": normal_values(streams_of[5], (FF, EMBED_WIDTH), FF ** -0.5, 0.125, ((0, 2),)),
        "level_query": draw_level_query(jax.random.fold_in(streams_of[11], 71), part),
        "w_dec_q": normal_values(streams_of[7], (EMBED_WIDTH, EMBED_WIDTH), EMBED_WIDTH ** -0.5, 0.25, ((1, 2),)),
        "w_dec_kv": normal_values(streams_of[8], (2, EMBED_WIDTH, EMBED_WIDTH), EMBED_WIDTH ** -0.5, 0.25, ((2, 2),)),
        "w_dec_o": normal_values(streams_of[9], (EMBED_WIDTH, EMBED_WIDTH), EMBED_WIDTH ** -0.5, 0.25, ((0, 2),)),
        "decode_matrix": normal_values(streams_of[10], (EMBED_WIDTH, TARGET_QUANTITY * SQUARE_SPAN * SQUARE_SPAN), EMBED_WIDTH ** -0.5, 0.25, (), jnp.float32),
    }


EPSILON = 1e-05

def layer_norm(values):
    center = values - lax.optimization_barrier(jnp.mean(values, axis=-1, keepdims=True))
    spread = lax.optimization_barrier(jnp.mean(center * center, axis=-1, keepdims=True))
    return center * lax.rsqrt(spread + EPSILON)

def window_attention(tile_tokens, key_marks, row_start, total_rows, w_qkv, w_proj):
    north_south_circles, columns, levels, features = tile_tokens.shape
    local_width = w_qkv.shape[2]
    head_count = local_width // HD
    normed = layer_norm(tile_tokens.astype(jnp.float32)).astype(jnp.bfloat16).reshape(-1, features)
    win_count = north_south_circles // WIN_LAT
    tok_count = WIN_LAT * columns * levels

    def project(which):
        result = jnp.dot(normed, w_qkv[which], preferred_element_type=jnp.float32)
        return result.astype(jnp.bfloat16).reshape(win_count, tok_count, head_count, HD)
    queries = project(0)
    key_heads = project(1)
    value_heads = project(2)
    scores = jnp.einsum('wqhd,wkhd->whqk', queries.astype(jnp.float32), key_heads.astype(jnp.float32)) * HD ** (-0.5)
    row_index = lax.broadcasted_iota(jnp.int32, (north_south_circles, columns, levels), 0).reshape(win_count, tok_count)
    region = row_index + row_start >= total_rows - WIN_LAT // 2
    open_key = jnp.broadcast_to(key_marks[:, :, None], (north_south_circles, columns, levels)).reshape(win_count, tok_count) > 0
    diagonal = lax.broadcasted_iota(jnp.int32, (tok_count, tok_count), 0) == lax.broadcasted_iota(jnp.int32, (tok_count, tok_count), 1)
    allowed = (region[:, :, None] == region[:, None, :]) & (open_key[:, None, :] | diagonal[None])
    scores = jnp.where(allowed[:, None], scores, jnp.float32(-1e+30))
    peak_score = lax.optimization_barrier(jnp.max(scores, axis=-1, keepdims=True))
    exp_scores = jnp.exp(scores - peak_score)
    weights = (exp_scores / lax.optimization_barrier(jnp.sum(exp_scores, axis=-1, keepdims=True))).astype(jnp.bfloat16)
    context = jnp.einsum('whqk,wkhd->wqhd', weights.astype(jnp.float32), value_heads.astype(jnp.float32))
    context = context.astype(jnp.bfloat16).reshape(-1, local_width)
    return jnp.dot(context, w_proj, preferred_element_type=jnp.float32).reshape(north_south_circles, columns, levels, features)

def level_decoder(latent, level_query, w_dec_q, w_dec_kv, w_dec_o):
    north_south_circles, columns, levels, features = latent.shape
    local_width = w_dec_kv.shape[2]
    head_count = local_width // HD
    patches = north_south_circles * columns
    normed = layer_norm(latent.astype(jnp.float32)).astype(jnp.bfloat16).reshape(-1, features)
    dkeys = jnp.dot(normed, w_dec_kv[0], preferred_element_type=jnp.float32).astype(jnp.bfloat16)
    dvals = jnp.dot(normed, w_dec_kv[1], preferred_element_type=jnp.float32).astype(jnp.bfloat16)
    dkeys = dkeys.reshape(patches, levels, head_count, HD)
    dvals = dvals.reshape(patches, levels, head_count, HD)
    dquery = jnp.dot(level_query, w_dec_q, preferred_element_type=jnp.float32).reshape(-1, head_count, HD)
    scores = jnp.einsum('lhd,pjhd->plhj', dquery, dkeys.astype(jnp.float32)) * HD ** (-0.5)
    peak_score = lax.optimization_barrier(jnp.max(scores, axis=-1, keepdims=True))
    exp_scores = jnp.exp(scores - peak_score)
    dweights = (exp_scores / lax.optimization_barrier(jnp.sum(exp_scores, axis=-1, keepdims=True))).astype(jnp.bfloat16)
    dcontext = jnp.einsum('plhj,pjhd->plhd', dweights.astype(jnp.float32), dvals.astype(jnp.float32))
    dcontext = dcontext.astype(jnp.bfloat16).reshape(-1, local_width)
    return jnp.dot(dcontext, w_dec_o, preferred_element_type=jnp.float32)

def reference(tokens, key_mask, w_qkv, w_proj, w_up, w_down, level_query, w_dec_q, w_dec_kv, w_dec_o, decode_matrix):
    north_south_circles, east_west_bands_set, levels, features = tokens.shape
    half_lat = WIN_LAT // 2
    half_lon = WINDOW_EASTWARD // 2
    block_count = east_west_bands_set // WINDOW_EASTWARD
    rolled = jnp.roll(tokens, (-half_lat, -half_lon), (0, 1))
    rolled_mask = jnp.roll(key_mask, (-half_lat, -half_lon), (0, 1))
    rolled = jnp.moveaxis(rolled.reshape(north_south_circles, block_count, WINDOW_EASTWARD, levels, features), 1, 0)
    rolled_mask = jnp.moveaxis(rolled_mask.reshape(north_south_circles, block_count, WINDOW_EASTWARD), 1, 0)

    def attend(block_pair):
        return window_attention(block_pair[0], block_pair[1], 0, north_south_circles, w_qkv, w_proj)
    attended = lax.map(attend, (rolled, rolled_mask))
    attended = jnp.moveaxis(attended, 0, 1).reshape(north_south_circles, east_west_bands_set, levels, features)
    attended = jnp.roll(attended, (half_lat, half_lon), (0, 1))
    x_one = tokens.astype(jnp.float32) + attended
    x_blocks = jnp.moveaxis(x_one.reshape(north_south_circles, block_count, WINDOW_EASTWARD, levels, features), 1, 0)

    def finish(x_block):
        normed = layer_norm(x_block).astype(jnp.bfloat16)
        hidden = jax.nn.gelu(jnp.dot(normed, w_up, preferred_element_type=jnp.float32), approximate=False).astype(jnp.bfloat16)
        latent = (x_block + jnp.dot(hidden, w_down, preferred_element_type=jnp.float32)).astype(jnp.bfloat16)
        dec_hidden = level_decoder(latent, level_query, w_dec_q, w_dec_kv, w_dec_o)
        cell_measures = jnp.dot(dec_hidden, decode_matrix, precision=lax.Precision.HIGHEST, preferred_element_type=jnp.float32)
        return cell_measures.reshape(north_south_circles, WINDOW_EASTWARD, ISOBAR_NUMBER, TARGET_QUANTITY, SQUARE_SPAN, SQUARE_SPAN)
    cell_measures = lax.map(finish, x_blocks)
    estimated_maps = jnp.transpose(cell_measures, (4, 3, 1, 5, 0, 2, 6))
    return estimated_maps.reshape(TARGET_QUANTITY, ISOBAR_NUMBER, north_south_circles * SQUARE_SPAN, east_west_bands_set * SQUARE_SPAN)
```

```python
import functools

import jax
import jax.numpy as jnp
from jax import lax
from jax.experimental import pallas as pl
from jax.experimental.pallas import tpu as pltpu
from jax.sharding import PartitionSpec as P

HD = 64
TARGET_QUANTITY = 4
ISOBAR_NUMBER = 13
SQUARE_SPAN = 4
WIN_LAT = 6
EPSILON = 1e-05
BLOCK = 128
LEVEL_STRIDE = 40
LEVEL_SLOTS = 16
NT = (((1,), (1,)), ((), ()))
F32 = jnp.float32
BF16 = jnp.bfloat16


def from_behind(shard, axis, by):
    peers = lax.axis_size(axis)
    return lax.ppermute(shard, axis, [(i, (i + by) % peers) for i in range(peers)])


def layer_norm(values):
    center = values - jnp.mean(values, axis=-1, keepdims=True)
    spread = jnp.mean(center * center, axis=-1, keepdims=True)
    return center * lax.rsqrt(spread + EPSILON)


def fold_kernel(lq_ref, wq_ref, wkv_ref, wo_ref, dm_ref, out_ref):
    width = wq_ref.shape[1]
    heads = width // HD
    dquery = jnp.dot(lq_ref[...], wq_ref[...], preferred_element_type=F32) * HD ** (-0.5)
    d_hi = dquery.astype(BF16)
    d_lo = (dquery - d_hi.astype(F32)).astype(BF16)
    slots = dquery.shape[0] * heads
    row = lax.broadcasted_iota(jnp.int32, (slots, dquery.shape[0]), 0)
    slot = lax.broadcasted_iota(jnp.int32, (slots, dquery.shape[0]), 1)
    spread = (row // heads == slot).astype(F32).astype(BF16)
    row = lax.broadcasted_iota(jnp.int32, (slots, width), 0)
    mine = row % heads == lax.broadcasted_iota(jnp.int32, (slots, width), 1) // HD
    q_hi = jnp.dot(spread, d_hi, preferred_element_type=F32)
    q_hi = jnp.where(mine, q_hi, 0.0).astype(BF16)
    q_lo = jnp.dot(spread, d_lo, preferred_element_type=F32)
    q_lo = jnp.where(mine, q_lo, 0.0).astype(BF16)
    wk = wkv_ref[0]
    g = lax.dot_general(q_hi, wk, NT, preferred_element_type=F32)
    g = g + lax.dot_general(q_lo, wk, NT, preferred_element_type=F32)
    g_hi = g.astype(BF16)
    count = g.shape[0]
    out_ref[0:count, :] = g_hi
    out_ref[count : 2 * count, :] = (g - g_hi.astype(F32)).astype(BF16)
    dm = dm_ref[...]
    dm_hi = dm.astype(BF16)
    dm_lo = (dm - dm_hi.astype(F32)).astype(BF16)
    wo = wo_ref[...]
    contract = (((0,), (1,)), ((), ()))
    m_t = lax.dot_general(dm_hi, wo, contract, preferred_element_type=F32)
    m_t = m_t + lax.dot_general(dm_lo, wo, contract, preferred_element_type=F32)
    pixels = m_t.shape[0]
    stacked = jnp.concatenate([m_t] * heads, axis=0)
    row_head = lax.broadcasted_iota(jnp.int32, stacked.shape, 0) // pixels
    lane_head = lax.broadcasted_iota(jnp.int32, stacked.shape, 1) // HD
    stacked = jnp.where(row_head == lane_head, stacked, 0.0)
    s_hi = stacked.astype(BF16)
    s_lo = (stacked - s_hi.astype(F32)).astype(BF16)
    wv = wkv_ref[1]
    n_t = lax.dot_general(s_hi, wv, NT, preferred_element_type=F32)
    n_t = n_t + lax.dot_general(s_lo, wv, NT, preferred_element_type=F32)
    out_ref[2 * count :, :] = n_t.astype(BF16)


def fold_decoder(level_query, w_dec_q, w_dec_kv, w_dec_o, decode_matrix):
    features = w_dec_q.shape[0]
    width = w_dec_q.shape[1]
    heads = width // HD
    padded = jnp.pad(level_query, ((0, LEVEL_SLOTS - level_query.shape[0]), (0, 0)))
    rows = heads * (2 * LEVEL_SLOTS + decode_matrix.shape[1])
    return pl.pallas_call(
        fold_kernel,
        out_shape=jax.ShapeDtypeStruct((rows, features), BF16),
        cost_estimate=pl.CostEstimate(flops=10**9, bytes_accessed=2 * 10**6, transcendentals=0),
    )(padded, w_dec_q, w_dec_kv, w_dec_o, decode_matrix)


def main_kernel(
    levels,
    own_ref,
    left_ref,
    right_ref,
    wqkv_a,
    wqkv_b,
    wproj_a,
    wproj_b,
    wup_a,
    wup_b,
    wdown_a,
    wdown_b,
    fold_a,
    fold_b,
    out_ref,
    n3_ref,
    dw_ref,
    u_ref,
):
    windows = left_ref.shape[0]
    features = own_ref.shape[-1]
    patches = LEVEL_STRIDE - 4
    last_core = lax.axis_index("var") == lax.axis_size("var") - 1
    width = wproj_a.shape[0]
    heads = width // HD

    q_pos = lax.broadcasted_iota(jnp.int32, (BLOCK, 2 * BLOCK), 0)
    k_pos = lax.broadcasted_iota(jnp.int32, (BLOCK, 2 * BLOCK), 1)
    diagonal = q_pos == k_pos
    k_pos = jnp.where(k_pos >= BLOCK, k_pos - BLOCK, k_pos)

    def region_of(pos):
        for level in range(levels - 1, 0, -1):
            pos = jnp.where(pos >= LEVEL_STRIDE * level, pos - LEVEL_STRIDE * level, pos)
        return pos >= patches // 2

    region_differs = region_of(q_pos) != region_of(k_pos)
    lane_head = lax.broadcasted_iota(jnp.int32, (BLOCK, width), 1) // HD

    @pl.loop(0, windows)
    def _(w):
        own = own_ref[w].reshape(2 * BLOCK, features)
        halo = jnp.concatenate([left_ref[w], right_ref[w]], axis=0)
        own_f = own.astype(F32)
        n_own = layer_norm(own_f).astype(BF16)
        n_halo = layer_norm(halo.astype(F32)).astype(BF16)
        cut = jnp.logical_and(w == windows - 1, last_core)
        marks_row = LEVEL_STRIDE - 1
        biases = []
        for half in range(2):
            own_open = own_f[half * BLOCK + marks_row : half * BLOCK + marks_row + 1, :BLOCK]
            halo_open = halo[half * BLOCK : half * BLOCK + LEVEL_STRIDE, :BLOCK].astype(F32)[
                marks_row : marks_row + 1
            ]
            open_key = jnp.concatenate([own_open, halo_open], axis=1) > 0.5
            allowed = jnp.logical_or(jnp.broadcast_to(open_key, diagonal.shape), diagonal)
            allowed = jnp.logical_and(
                allowed, jnp.logical_not(jnp.logical_and(region_differs, cut))
            )
            biases.append(jnp.where(allowed, 0.0, -1e30))
        attended = jnp.zeros((2 * BLOCK, features), F32)
        for wqkv, wproj in ((wqkv_a, wproj_a), (wqkv_b, wproj_b)):
            q = jnp.dot(n_own, wqkv[0], preferred_element_type=F32)
            q = (q.astype(BF16).astype(F32) * HD ** (-0.5)).astype(BF16)
            k_own = jnp.dot(n_own, wqkv[1], preferred_element_type=F32).astype(BF16)
            v_own = jnp.dot(n_own, wqkv[2], preferred_element_type=F32).astype(BF16)
            k_halo = jnp.dot(n_halo, wqkv[1], preferred_element_type=F32).astype(BF16)
            v_halo = jnp.dot(n_halo, wqkv[2], preferred_element_type=F32).astype(BF16)
            parts = []
            for half in range(2):
                at = slice(half * BLOCK, (half + 1) * BLOCK)
                keys = jnp.concatenate([k_own[at], k_halo[at]], axis=0)
                vals = jnp.concatenate([v_own[at], v_halo[at]], axis=0)
                qh = q[at]
                context = jnp.zeros((BLOCK, width), F32)
                for h in range(heads):
                    q_one = jnp.where(lane_head == h, qh, jnp.zeros_like(qh))
                    s = lax.dot_general(q_one, keys, NT, preferred_element_type=F32)
                    s = s + biases[half]
                    peak = jnp.max(s, axis=-1, keepdims=True)
                    e = jnp.exp(s - peak)
                    total = jnp.sum(e, axis=-1, keepdims=True)
                    o = jnp.dot(e.astype(BF16), vals, preferred_element_type=F32)
                    context = jnp.where(lane_head == h, o / total, context)
                parts.append(context.astype(BF16))
            context = jnp.concatenate(parts, axis=0)
            attended = attended + jnp.dot(context, wproj[...], preferred_element_type=F32)
        x_one = own_f + attended
        n2 = layer_norm(x_one).astype(BF16)
        latent = x_one
        for wup, wdown in ((wup_a, wdown_a), (wup_b, wdown_b)):
            for c in range(0, wup.shape[1], 256):
                hid = jnp.dot(n2, wup[:, c : c + 256], preferred_element_type=F32)
                hid = 0.5 * hid * (1.0 + lax.erf(hid * 2.0 ** (-0.5)))
                latent = latent + jnp.dot(
                    hid.astype(BF16), wdown[c : c + 256, :], preferred_element_type=F32
                )
        n3 = layer_norm(latent.astype(BF16).astype(F32))
        for half in range(2):
            for level in range(levels):
                start = half * BLOCK + level * LEVEL_STRIDE
                n3_ref[level, w * 2 + half] = n3[start : start + LEVEL_STRIDE]

    total_patches = windows * 2 * LEVEL_STRIDE
    padded = dw_ref.shape[-1]
    count = heads * LEVEL_SLOTS
    pixels = u_ref.shape[1] // (2 * heads)
    for j in range(levels):
        n3 = n3_ref[j].reshape(total_patches, features).astype(BF16)
        n3 = jnp.concatenate(
            [n3, jnp.zeros((padded - total_patches, features), BF16)], axis=0
        )
        for s, fold in enumerate((fold_a, fold_b)):
            g = lax.dot_general(fold[0 : 2 * count, :], n3, NT, preferred_element_type=F32)
            dw_ref[j, s * count : (s + 1) * count, :] = g[:count] + g[count:]
            u_ref[j, s * heads * pixels : (s + 1) * heads * pixels, :] = lax.dot_general(
                fold[2 * count :, :], n3, NT, preferred_element_type=F32
            )
    scores = [dw_ref[j] for j in range(levels)]
    peak = functools.reduce(jnp.maximum, scores)
    e = [jnp.exp(s - peak) for s in scores]
    inverse = 1.0 / sum(e)
    for j in range(levels):
        dw_ref[j] = (e[j] * inverse).astype(BF16).astype(F32)

    pair = 8 // heads

    @pl.loop(0, out_ref.shape[0] // pair)
    def _(group):
        for c in range(0, padded, BLOCK):
            totals = [jnp.zeros((pixels, BLOCK), F32) for _ in range(pair)]
            for s in range(2):
                for j in range(levels):
                    start = pl.multiple_of(s * count + group * 8, 8)
                    weights = dw_ref[j, pl.ds(start, 8), c : c + BLOCK]
                    for h in range(heads):
                        top = (s * heads + h) * pixels
                        value = u_ref[j, top : top + pixels, c : c + BLOCK]
                        for n in range(pair):
                            totals[n] = totals[n] + weights[n * heads + h : n * heads + h + 1] * value
            for n in range(pair):
                out_ref[group * pair + n, :, c : c + BLOCK] = totals[n].astype(BF16)


def local(
    tokens,
    key_mask,
    w_qkv,
    w_proj,
    w_up,
    w_down,
    level_query,
    w_dec_q,
    w_dec_kv,
    w_dec_o,
    decode_matrix,
):
    all_rows, columns, levels, features = tokens.shape
    half_cols = columns // 2
    half_lat = WIN_LAT // 2
    cores = lax.axis_size("var")
    row_count = all_rows // cores
    windows = row_count // WIN_LAT
    patches = WIN_LAT * half_cols
    row_start = lax.axis_index("var") * row_count

    rows = lax.dynamic_slice_in_dim(jnp.roll(tokens, -half_lat, 0), row_start, row_count, 0)
    marks = lax.dynamic_slice_in_dim(jnp.roll(key_mask, -half_lat, 0), row_start, row_count, 0)
    own = rows.reshape(windows, WIN_LAT, 2, half_cols, levels, features)
    own = jnp.transpose(own, (2, 0, 4, 1, 3, 5)).reshape(2, windows, levels, patches, features)
    marks = marks.reshape(windows, WIN_LAT, 2, half_cols).transpose(2, 0, 1, 3)
    marks = (marks > 0).astype(BF16).reshape(2, windows, 1, patches)
    marks = jnp.pad(marks, ((0, 0), (0, 0), (0, 0), (0, LEVEL_STRIDE - patches)))
    marks = jnp.tile(marks, (1, 1, 1, levels))
    marks = jnp.pad(marks, ((0, 0), (0, 0), (0, 0), (0, features - levels * LEVEL_STRIDE)))
    own = jnp.pad(own, ((0, 0), (0, 0), (0, 0), (0, LEVEL_STRIDE - 1 - patches), (0, 0)))
    marks = jnp.broadcast_to(marks[:, :, None], (2, windows, levels, 1, features))
    own = jnp.concatenate([own, marks], axis=3)
    own = own.reshape(2, windows, levels * LEVEL_STRIDE, features)
    own = jnp.pad(own, ((0, 0), (0, 0), (0, BLOCK - levels * LEVEL_STRIDE), (0, 0)))
    right = from_behind(own[0], "grid", -1)
    left = from_behind(own[1], "grid", 1)

    other = [from_behind(w, "var", 1) for w in (w_qkv, w_proj, w_up, w_down)]
    fold = fold_decoder(level_query, w_dec_q, w_dec_kv, w_dec_o, decode_matrix)
    fold_other = from_behind(fold, "var", 1)

    out_pixels = decode_matrix.shape[1]
    isobars = level_query.shape[0]
    heads_all = cores * (w_proj.shape[0] // HD)
    padded = -(-windows * 2 * LEVEL_STRIDE // BLOCK) * BLOCK
    pixels = pl.pallas_call(
        functools.partial(main_kernel, levels),
        out_shape=jax.ShapeDtypeStruct((isobars + isobars % 2, out_pixels, padded), BF16),
        scratch_shapes=[
            pltpu.VMEM((levels, windows * 2, LEVEL_STRIDE, features), F32),
            pltpu.VMEM((levels, heads_all * LEVEL_SLOTS, padded), F32),
            pltpu.VMEM((levels, heads_all * out_pixels, padded), F32),
        ],
        compiler_params=pltpu.CompilerParams(vmem_limit_bytes=60 * 2**20),
    )(
        jnp.transpose(own, (1, 0, 2, 3)),
        left,
        right,
        w_qkv,
        other[0],
        w_proj,
        other[1],
        w_up,
        other[2],
        w_down,
        other[3],
        fold,
        fold_other,
    )
    return exchange(pixels, row_count, columns, isobars)


def exchange(pixels, row_count, columns, isobars):
    half_cols = columns // 2
    half_lat = WIN_LAT // 2
    windows = row_count // WIN_LAT
    patches = WIN_LAT * half_cols
    pixels = pixels[:isobars, :, : windows * 2 * LEVEL_STRIDE]
    pixels = pixels.reshape(
        isobars, TARGET_QUANTITY, SQUARE_SPAN, SQUARE_SPAN, windows, 2, LEVEL_STRIDE
    )[..., :patches]
    pixels = pixels.reshape(
        isobars, TARGET_QUANTITY, SQUARE_SPAN, SQUARE_SPAN, windows, 2, WIN_LAT, half_cols
    )
    pixels = jnp.transpose(pixels, (1, 0, 4, 6, 2, 5, 7, 3))
    maps = pixels.reshape(
        TARGET_QUANTITY, isobars, row_count * SQUARE_SPAN, columns * SQUARE_SPAN
    )
    maps = lax.all_to_all(maps, "var", split_axis=0, concat_axis=2, tiled=True)
    maps = jnp.roll(maps, half_lat * SQUARE_SPAN, 2)
    maps = lax.all_to_all(maps, "grid", split_axis=2, concat_axis=3, tiled=True)
    return maps.astype(F32)


def solution(mesh):
    placed = (
        P("group", "grid", None, None),
        P("group", "grid"),
        P(None, None, "var"),
        P("var", None),
        P(None, "var"),
        P("var", None),
        P(),
        P(None, "var"),
        P(None, None, "var"),
        P("var", None),
        P(),
    )
    return jax.shard_map(
        local,
        mesh=mesh,
        in_specs=placed,
        out_specs=P("var", "group", "grid", None),
        check_vma=False,
    )
```
